128 devices in a mesh: row: 16 (over z, y_hi, core), col: 8 (over y_lo, x).
Axes of the slice: x: 4, y: 4 (y_hi: 2, y_lo: 2; y = y_hi * 2 + y_lo), z: 4, core: 2. Of those that a mesh axis runs over, the one named last changes fastest.
Arguments:
- left_prop: float32 [16, 8, 2, 512, 512], P('row', None, None, 'col'), may hold values from -0.1875 to 0.1875
- vertex: float32 [8, 2, 512, 512], P(None, None, ('row', 'col')), may hold values from -5 to 5
- right_prop: float32 [8, 16, 2, 512, 512], P(None, 'col', None, None, 'row'), may hold values from -0.1875 to 0.1875
- insertions: int32 [3], replicated, may hold values from 0 to 7
- window_start: int32 [2], replicated, may hold values from 0 to 255
Outputs:
- correlator: float32 [16, 16, 2, 512, 512], P('row', 'col')
The draws below stay inside these ranges and needn't reach their ends.
Inputs may be any that keep to these rules, and one draw needn't show every extreme that they name: `insertions`: repeats may occur.
All inputs are finite; a program needn't handle non-finite values.
Results may differ from the reference program's by a relative error of at most 0.0001.
Values sent between devices are 32-bit elements; how exact they have to be, the bound alone decides.
No kernel may reach another device: no remote copies, remote signals or barrier semaphores. Data moves between devices by JAX's collectives and lax.ppermute only.
A program may use at most 128 MiB of HBM per device.

```python
import jax
import jax.numpy as jnp
from jax import lax

NS = 8
LT = 256
INSERTS = 3
M = 512
T_SRC = 16
T_SNK = 16


def shard_levels(own_key, extent, shards, smallest, largest):
    def one(dim, blocks):
        steps = jax.random.uniform(jax.random.fold_in(jax.random.fold_in(own_key, 6), dim), (blocks,), jnp.float32, smallest / len(shards), largest / len(shards))
        return jnp.repeat(jnp.exp(steps), extent[dim] // blocks).reshape((-1,) + (1,) * (len(extent) - dim - 1))

    gain = one(*shards[0])
    for cut in shards[1:]:
        gain = gain * one(*cut)
    return gain


def bell_draw(rng, dims, deviation, bound, shards=(), kind=jnp.bfloat16):
    entries = jax.random.normal(rng, dims, jnp.float32) * deviation
    if len(shards) > 0:
        entries = shard_levels(rng, dims, shards, -0.22, 0.18) * entries
    return jnp.clip(entries, min=-bound, max=bound).astype(kind)


def setup_inputs(seed: int = 0) -> dict:
    key_of = jax.random.split(jax.random.key(seed), 6)
    return {
        "left_prop": bell_draw(key_of[0], (T_SRC, NS, 2, M, M), (2 * M) ** -0.5, 0.1875, ((0, 16), (3, 8)), jnp.float32),
        "vertex": bell_draw(key_of[1], (NS, 2, M, M), 0.7071, 5.0, ((2, 128),), jnp.float32),
        "right_prop": bell_draw(key_of[2], (NS, T_SNK, 2, M, M), (2 * M) ** -0.5, 0.1875, ((1, 8), (4, 16)), jnp.float32),
        "insertions": jax.random.randint(key_of[3], (INSERTS,), 0, NS).astype(jnp.int32),
        "window_start": jax.random.randint(key_of[4], (2,), 0, LT).astype(jnp.int32),
    }


def complex_product(first, second):
    highest = lax.Precision.HIGHEST
    first_re, first_im = first[..., 0, :, :], first[..., 1, :, :]
    second_re, second_im = second[..., 0, :, :], second[..., 1, :, :]
    real_part = jnp.matmul(first_re, second_re, precision=highest) - jnp.matmul(first_im, second_im, precision=highest)
    imag_part = jnp.matmul(first_re, second_im, precision=highest) + jnp.matmul(first_im, second_re, precision=highest)
    return jnp.stack([real_part, imag_part], axis=-3)


def boundary_signs(insertions, window_start, source_slots, sink_slots):
    slice_times = insertions * (LT // NS)
    source_times = (window_start[0] + source_slots) % LT
    sink_times = (window_start[1] + sink_slots) % LT
    left_sign = jnp.where(slice_times[None, :] < source_times[:, None], -1.0, 1.0).astype(jnp.float32)
    right_sign = jnp.where(sink_times[None, :] < slice_times[:, None], -1.0, 1.0).astype(jnp.float32)
    return left_sign, right_sign


def reference(left_prop, vertex, right_prop, insertions, window_start):
    source_slots = jnp.arange(T_SRC, dtype=jnp.int32)
    sink_slots = jnp.arange(T_SNK, dtype=jnp.int32)
    left_sign, right_sign = boundary_signs(insertions, window_start, source_slots, sink_slots)
    chosen_left = jnp.take(left_prop, insertions, axis=1) * left_sign[:, :, None, None, None]
    vertex_full = jnp.take(vertex, insertions, axis=0)
    chosen_right = jnp.take(right_prop, insertions, axis=0) * right_sign[:, :, None, None, None]

    def one_source(left_blocks):
        through = complex_product(left_blocks, vertex_full)
        summed = jnp.zeros((T_SNK, 2, M, M), jnp.float32)
        for which in range(INSERTS):
            summed = summed + complex_product(through[which][None], chosen_right[which])
        return summed

    return lax.map(one_source, chosen_left)
```

```python
import jax
import jax.numpy as jnp
import numpy as np
from jax import lax
from jax.experimental import pallas as pl
from jax.experimental.pallas import tpu as pltpu
from jax.sharding import Mesh
from jax.sharding import PartitionSpec as P

NS = 8
LT = 256
AXES = ("z", "h", "c", "l", "x")
SIZES = (4, 2, 2, 2, 4)
ROW = ("z", "h", "c")
COL = ("l", "x")
F32 = jnp.float32
BF16 = jnp.bfloat16


def shift(value, **step):
    index = np.arange(128).reshape(SIZES)
    pairs = []
    for place in np.ndindex(*SIZES):
        goal = tuple((p + step.get(a, 0)) % s for p, a, s in zip(place, AXES, SIZES))
        pairs.append((int(index[place]), int(index[goal])))
    return lax.ppermute(value, AXES, pairs)


def ring_pair(own, ring, pair):
    up, down = {ring: 1}, {ring: 3}
    got = {(0, 0): own}
    got[0, 1] = shift(own, **up)
    got[0, 3] = shift(own, **down)
    got[1, 0] = shift(own, **{pair: 1})
    got[1, 1] = shift(got[1, 0], **up)
    got[1, 3] = shift(got[1, 0], **down)
    got[0, 2] = shift(got[0, 1], **up)
    got[1, 2] = shift(got[1, 3], **down)
    return got


def limbs(value):
    high = value.astype(BF16)
    return high, (value - high.astype(F32)).astype(BF16)


def vertex_kernel(pos, *refs):
    pieces, (high, low) = refs[:8], refs[8:]
    z, h, c, l = pos[0], pos[1], pos[2], pos[3]
    for n, piece in enumerate(pieces):
        dc, dh, dl = n // 4, n // 2 % 2, n % 2
        base = lax.rem(h + dh, 2) * 4 + lax.rem(c + dc, 2) * 2 + lax.rem(l + dl, 2)

        def one(dz, carry):
            row = pl.multiple_of((lax.rem(z + 4 - dz, 4) * 8 + base) * 16, 16)
            for k in range(3):
                re, im = piece[dz, k, 0], piece[dz, k, 1]
                for g, value in enumerate((re, im, re + im)):
                    high[k, g, pl.ds(row, 16), :], low[k, g, pl.ds(row, 16), :] = limbs(value)
            return carry

        lax.fori_loop(0, 4, one, 0)


def nn(a, b):
    return lax.dot_general(a, b, (((1,), (0,)), ((), ())), preferred_element_type=F32)


def nt(a, b):
    return lax.dot_general(a, b, (((1,), (1,)), ((), ())), preferred_element_type=F32)


def left_kernel(*refs):
    pieces, (vh, vl, high, low) = refs[:-4], refs[-4:]
    for k in range(3):
        re = jnp.concatenate([p[k, 0] for p in pieces], axis=0)
        im = jnp.concatenate([p[k, 1] for p in pieces], axis=0)
        out = []
        for g, value in enumerate((re, im, re + im)):
            a_h, a_l = limbs(value)
            out.append(nn(a_h, vh[k, g]) + nn(a_h, vl[k, g]) + nn(a_l, vh[k, g]))
        re = out[0] - out[1]
        im = out[2] - out[0] - out[1]
        for g, value in enumerate((re, im, re + im)):
            high[g, :, k * 512 : (k + 1) * 512], low[g, :, k * 512 : (k + 1) * 512] = limbs(value)


def sink_kernel(dz, rows, pos, high, low, *refs):
    pieces = refs[:4]
    out, bh, bl, slab, sem = refs[-5:]
    z, h, c, l, x = (pos[n] for n in range(5))
    for n, piece in enumerate(pieces):
        dc, dh = n // 2, n % 2
        q = lax.rem(h + dh, 2) * 2 + lax.rem(c + dc, 2)
        for u in range(2):
            row = pl.multiple_of(u * 128 + q * 32, 32)
            for k in range(3):
                re, im = piece[k, u, 0], piece[k, u, 1]
                for g, value in enumerate((re, im, re + im)):
                    span = slice(k * 512, (k + 1) * 512)
                    bh[g, pl.ds(row, 32), span], bl[g, pl.ds(row, 32), span] = limbs(value)
    prod = []
    for g in range(3):
        prod.append(nt(high[g], bh[g]) + nt(high[g], bl[g]) + nt(low[g], bh[g]))
    re = prod[0] - prod[1]
    im = prod[2] - prod[0] - prod[1]
    for n, (dl, dx) in enumerate(rows):
        block = lax.rem(l + dl, 2) * 4 + lax.rem(x + 4 - dx, 4)
        span = pl.ds(pl.multiple_of(block * 64, 64), 64)
        for u in range(2):
            slab[u, 0, span, :] = re[n * 64 : (n + 1) * 64, u * 128 : (u + 1) * 128]
            slab[u, 1, span, :] = im[n * 64 : (n + 1) * 64, u * 128 : (u + 1) * 128]
    lane = pl.multiple_of(lax.rem(z + 4 - dz, 4) * 128, 128)
    copy = pltpu.make_async_copy(slab, out.at[:, :, :, pl.ds(lane, 128)], sem)
    copy.start()
    copy.wait()


VM = pl.BlockSpec(memory_space=pltpu.VMEM)
SM = pl.BlockSpec(memory_space=pltpu.SMEM)
ANY = pl.BlockSpec(memory_space=pl.ANY)


def cost(flops, data):
    return pl.CostEstimate(flops=flops, bytes_accessed=data, transcendentals=0)


def per_device(left_prop, vertex, right_prop, insertions, window_start):
    coords = {a: lax.axis_index(a) for a in AXES}
    pos = jnp.stack([coords[a] for a in AXES]).astype(jnp.int32)
    source = lax.axis_index(ROW)
    sinks = lax.axis_index(COL) * 2 + jnp.arange(2, dtype=jnp.int32)
    slice_times = insertions * (LT // NS)
    source_time = (window_start[0] + source) % LT
    sink_times = (window_start[1] + sinks) % LT
    left_sign = jnp.where(slice_times < source_time, -1.0, 1.0).astype(F32)
    right_sign = jnp.where(sink_times[None, :] < slice_times[:, None], -1.0, 1.0).astype(F32)
    left = jnp.take(left_prop[0], insertions, axis=0) * left_sign[:, None, None, None]
    right = jnp.take(right_prop, insertions, axis=0) * right_sign[:, :, None, None, None]
    right = jnp.swapaxes(right, -1, -2)
    vert = jnp.take(vertex, insertions, axis=0)

    part = [vert, shift(vert, x=3), shift(vert, x=2), shift(vert, x=1)]
    x = coords["x"]
    slots = []
    for j in range(4):
        pick = part[3]
        for e in range(3):
            pick = jnp.where((x + e) % 4 == j, part[e], pick)
        slots.append(pick)
    rows16 = jnp.concatenate(slots, axis=2)
    zs = jnp.stack([rows16, shift(rows16, z=1), shift(rows16, z=2), shift(rows16, z=3)])
    near = shift(zs, l=1)
    across = {(0, 0): zs, (0, 1): near, (1, 1): shift(zs, h=1, l=1), (1, 0): shift(near, h=1, l=1)}
    vert_pieces = [across[dh, dl] for dh in range(2) for dl in range(2)]
    vert_pieces += [shift(p, c=1) for p in vert_pieces]

    lefts = ring_pair(left, "x", "l")
    rights = ring_pair(right, "z", "h")
    others = {key: shift(p, c=1) for key, p in rights.items()}

    limb = jax.ShapeDtypeStruct((3, 3, 512, 512), BF16)
    vh, vl = pl.pallas_call(
        vertex_kernel,
        out_shape=[limb, limb],
        in_specs=[SM] + [VM] * 8,
        out_specs=[VM, VM],
        compiler_params=pltpu.CompilerParams(vmem_limit_bytes=24 << 20),
        cost_estimate=cost(10**8, 16 << 20),
        name="vertex_limbs",
    )(pos, *vert_pieces)

    rows = [(0, 0), (1, 0), (0, 1), (0, 3), (1, 1), (1, 3), (0, 2), (1, 2)]
    side = jax.ShapeDtypeStruct((3, 512, 1536), BF16)
    high, low = pl.pallas_call(
        left_kernel,
        out_shape=[side, side],
        in_specs=[VM] * 10,
        out_specs=[VM, VM],
        compiler_params=pltpu.CompilerParams(vmem_limit_bytes=48 << 20),
        cost_estimate=cost(9 * 3 * 2 * 512**3, 24 << 20),
        name="left_vertex",
    )(*[lefts[r] for r in rows], vh, vl)

    out = None
    for dz in (0, 1, 3, 2):
        pieces = [rights[0, dz], rights[1, dz], others[0, dz], others[1, dz]]
        body = lambda *refs, dz=dz: sink_kernel(dz, rows, *refs)
        extra = [] if out is None else [out]
        out = pl.pallas_call(
            body,
            out_shape=jax.ShapeDtypeStruct((2, 2, 512, 512), F32),
            in_specs=[SM] + [VM] * 6 + [ANY] * len(extra),
            out_specs=ANY,
            scratch_shapes=[
                pltpu.VMEM((3, 256, 1536), BF16),
                pltpu.VMEM((3, 256, 1536), BF16),
                pltpu.VMEM((2, 2, 512, 128), F32),
                pltpu.SemaphoreType.DMA,
            ],
            input_output_aliases={7: 0} if extra else {},
            compiler_params=pltpu.CompilerParams(vmem_limit_bytes=40 << 20),
            cost_estimate=cost(9 * 3 * 2 * 256 * 512**2, 14 << 20),
            name="sink_block",
        )(pos, high, low, *pieces, *extra)
    return out[None]


def solution(mesh):
    finer = Mesh(mesh.devices.reshape(SIZES), AXES)
    return jax.shard_map(
        per_device,
        mesh=finer,
        in_specs=(
            P(ROW, None, None, COL, None),
            P(None, None, AXES, None),
            P(None, COL, None, None, ROW),
            P(),
            P(),
        ),
        out_specs=P(ROW, COL, None, None, None),
        check_vma=False,
    )
```

```python
import functools

import jax
import jax.numpy as jnp
import numpy as np
from jax import lax
from jax.experimental import pallas as pl
from jax.experimental.pallas import tpu as pltpu
from jax.sharding import Mesh
from jax.sharding import PartitionSpec as P


NS = 8
LT = 256
AXES = ("z", "h", "c", "l", "x")
SIZES = (4, 2, 2, 2, 4)
ROW = ("z", "h", "c")
COL = ("l", "x")
F32 = jnp.float32
BF16 = jnp.bfloat16


GROUPS = ((0,), (1,), (3,), (2,))
LEFT_LIMIT = 26
SINK_LIMIT = 17


def shift(value, step):
    index = np.arange(128).reshape(SIZES)
    pairs = []
    for place in np.ndindex(*SIZES):
        goal = tuple((p + step.get(a, 0)) % s for p, a, s in zip(place, AXES, SIZES))
        pairs.append((int(index[place]), int(index[goal])))
    return lax.ppermute(value, AXES, pairs)


def select_kernel(chosen, left, vertex, right, left_out, vertex_out, right_out, sems):
    copies = []
    for k in range(3):
        for n, (src, dst) in enumerate(((vertex, vertex_out), (right, right_out), (left, left_out))):
            copies.append(pltpu.make_async_copy(src.at[chosen[k]], dst.at[k], sems.at[k, n]))
    for copy in copies:
        copy.start()
    for copy in copies:
        copy.wait()


def limbs(value):
    high = value.astype(BF16)
    return high, (value - high.astype(F32)).astype(BF16)


def nn(a, b):
    return lax.dot_general(a, b, (((1,), (0,)), ((), ())), preferred_element_type=F32)


def nt(a, b):
    return lax.dot_general(a, b, (((1,), (1,)), ((), ())), preferred_element_type=F32)


def left_kernel(rows, pos, *refs):
    verts, lefts, (high, low, vh, vl) = refs[:8], refs[8:16], refs[16:]
    z, h, c, l, x = (pos[n] for n in range(5))
    spots = []
    for dl, dx in rows:
        block = lax.rem(l + dl, 2) * 4 + lax.rem(x + 4 - dx, 4)
        spots.append(pl.ds(pl.multiple_of(block * 64, 64), 64))
    for k in range(3):
        for n, piece in enumerate(verts):
            core, d3 = lax.rem(c + n // 4, 2), n % 4

            def split(d2, carry):
                group = lax.rem(z + 4 - d2, 4) * 8 + lax.rem(h + d3 // 2, 2) * 4 + core * 2
                row = pl.multiple_of((group + lax.rem(l + d3 % 2, 2)) * 16, 16)
                re, im = (
                    jnp.concatenate([piece[d2, lax.rem(x + 4 - j, 4), k, g] for j in range(4)], axis=0)
                    for g in range(2)
                )
                for g, value in enumerate((re, im, re + im)):
                    vh[g, pl.ds(row, 16), :], vl[g, pl.ds(row, 16), :] = limbs(value)
                return carry

            lax.fori_loop(0, 4, split, 0, unroll=True)
        re = jnp.concatenate([piece[k, 0] for piece in lefts], axis=0)
        im = jnp.concatenate([piece[k, 1] for piece in lefts], axis=0)
        lhs = [limbs(value) for value in (re, im, re + im)]
        for n in range(0, 512, 256):
            cols = slice(n, n + 256)
            prod = []
            for g, (a_h, a_l) in enumerate(lhs):
                v_h, v_l = vh[g, :, cols], vl[g, :, cols]
                prod.append(nn(a_h, v_h) + nn(a_h, v_l) + nn(a_l, v_h))
            re = prod[0] - prod[1]
            im = prod[2] - prod[0] - prod[1]
            span = slice(k * 512 + n, k * 512 + n + 256)
            for g, value in enumerate((re, im, re + im)):
                value_h, value_l = limbs(value)
                for m, spot in enumerate(spots):
                    high[g, spot, span] = value_h[m * 64 : (m + 1) * 64]
                    low[g, spot, span] = value_l[m * 64 : (m + 1) * 64]


def sink_prepare(pos, sign, pieces, bh, bl):
    h, c = pos[1], pos[2]
    for m, piece in enumerate(pieces):
        q = lax.rem(h + m % 2, 2) * 2 + lax.rem(c + m // 2, 2)
        for u in range(2):
            row = pl.ds(pl.multiple_of(u * 128 + q * 32, 32), 32)
            for k in range(3):
                re, im = piece[k, u, 0] * sign[k, u], piece[k, u, 1] * sign[k, u]
                span = slice(k * 512, (k + 1) * 512)
                for g, value in enumerate((re, im, re + im)):
                    bh[g, row, span], bl[g, row, span] = limbs(value)


def sink_product(high, low, bh, bl, slab):
    prod = []
    for g in range(3):
        prod.append(nt(high[g], bh[g]) + nt(high[g], bl[g]) + nt(low[g], bh[g]))
    re = prod[0] - prod[1]
    im = prod[2] - prod[0] - prod[1]
    for u in range(2):
        slab[u, 0] = re[:, u * 128 : (u + 1) * 128]
        slab[u, 1] = im[:, u * 128 : (u + 1) * 128]


def sink_kernel(dz, pos, sign, high, low, *refs):
    out, bh, bl, slab, sem = refs[-5:]
    sink_prepare(pos, sign, refs[:4], bh, bl)
    sink_product(high, low, bh, bl, slab)
    lane = pl.multiple_of(lax.rem(pos[0] + 4 - dz, 4) * 128, 128)
    copy = pltpu.make_async_copy(slab, out.at[:, :, :, pl.ds(lane, 128)], sem)
    copy.start()
    copy.wait()


VM = pl.BlockSpec(memory_space=pltpu.VMEM)
SM = pl.BlockSpec(memory_space=pltpu.SMEM)
ANY = pl.BlockSpec(memory_space=pl.ANY)
HB = pl.BlockSpec(memory_space=pltpu.HBM)
HB = pl.BlockSpec(memory_space=pltpu.HBM)


LEFT_SCRATCH = [pltpu.VMEM((3, 512, 512), BF16), pltpu.VMEM((3, 512, 512), BF16)]
SINK_SCRATCH = [pltpu.VMEM((3, 256, 1536), BF16) for _ in range(2)]
SINK_SCRATCH += [pltpu.VMEM((2, 2, 512, 128), F32), pltpu.SemaphoreType.DMA]


def cost(flops, data):
    return pl.CostEstimate(flops=flops, bytes_accessed=data, transcendentals=0)


def contract(left_prop, vertex, right_prop, insertions, window_start):
    coords = {a: lax.axis_index(a) for a in AXES}
    pos = jnp.stack([coords[a] for a in AXES]).astype(jnp.int32)
    source = lax.axis_index(ROW)
    sinks = lax.axis_index(COL) * 2 + jnp.arange(2, dtype=jnp.int32)
    slice_times = insertions * (LT // NS)
    source_time = (window_start[0] + source) % LT
    sink_times = (window_start[1] + sinks) % LT
    left_sign = jnp.where(slice_times < source_time, -1.0, 1.0).astype(F32)
    right_sign = jnp.where(sink_times[None, :] < slice_times[:, None], -1.0, 1.0).astype(F32)
    sign = right_sign * left_sign[:, None]
    left, vert, right = pl.pallas_call(
        select_kernel,
        out_shape=[
            jax.ShapeDtypeStruct((3, 2, 64, 512), F32),
            jax.ShapeDtypeStruct((3, 2, 4, 512), F32),
            jax.ShapeDtypeStruct((3, 2, 2, 32, 512), F32),
        ],
        in_specs=[SM, HB, HB, HB],
        out_specs=[VM, VM, VM],
        scratch_shapes=[pltpu.SemaphoreType.DMA((3, 3))],
        compiler_params=pltpu.CompilerParams(vmem_limit_bytes=60 << 20),
        name="select",
    )(insertions, left_prop[0], vertex, jnp.swapaxes(right_prop, -1, -2))

    near, far, cross = dict(l=1), dict(h=1, l=1), dict(h=1)
    part = {0: vert}
    for d in (1, 3, 2):
        part[d] = shift(vert, dict(x=d))
    v1 = jnp.stack([part[d] for d in range(4)])
    part = {0: v1}
    for d in (1, 3, 2):
        part[d] = shift(v1, dict(z=d))
    v2 = jnp.stack([part[d] for d in range(4)])
    part = {0: v2}
    for d, way in ((1, near), (3, far), (2, cross)):
        part[d] = shift(v2, way)
    vert_pieces = [part[d] for d in range(4)]
    vert_pieces += [shift(part[d], dict(c=1)) for d in range(4)]

    lefts = {(0, 0): left}
    lefts[0, 1] = shift(left, dict(x=1))
    lefts[0, 3] = shift(left, dict(x=3))
    lefts[1, 0] = shift(left, dict(l=1))
    lefts[1, 1] = shift(lefts[1, 0], dict(x=1))
    lefts[1, 3] = shift(lefts[1, 0], dict(x=3))
    lefts[0, 2] = shift(lefts[0, 1], dict(x=1))
    lefts[1, 2] = shift(lefts[1, 3], dict(x=3))
    rights = {(0, 0): right}
    rights[0, 1] = shift(right, dict(z=1))
    rights[0, 3] = shift(right, dict(z=3))
    rights[1, 0] = shift(right, dict(h=1))
    rights[1, 1] = shift(rights[1, 0], dict(z=1))
    rights[1, 3] = shift(rights[1, 0], dict(z=3))
    rights[0, 2] = shift(rights[0, 1], dict(z=1))
    rights[1, 2] = shift(rights[1, 3], dict(z=3))
    others = {key: shift(p, dict(c=1)) for key, p in rights.items()}

    def chunk(dz):
        return [rights[0, dz], rights[1, dz], others[0, dz], others[1, dz]]

    rows = [(0, 0), (1, 0), (0, 1), (0, 3), (1, 1), (1, 3), (0, 2), (1, 2)]
    side = jax.ShapeDtypeStruct((3, 512, 1536), BF16)
    whole_out = jax.ShapeDtypeStruct((2, 2, 512, 512), F32)
    high, low = pl.pallas_call(
        functools.partial(left_kernel, rows),
        out_shape=[side, side],
        in_specs=[SM] + [VM] * 16,
        out_specs=[VM, VM],
        scratch_shapes=LEFT_SCRATCH,
        compiler_params=pltpu.CompilerParams(vmem_limit_bytes=LEFT_LIMIT << 20),
        cost_estimate=cost(9 * 3 * 2 * 512**3, 24 << 20),
        name="left_vertex",
    )(pos, *vert_pieces, *[lefts[r] for r in rows])

    out = None
    for steps in GROUPS:
        pieces = [p for dz in steps for p in chunk(dz)]
        extra = [] if out is None else [out]
        out = pl.pallas_call(
            functools.partial(sink_kernel, steps[0]),
            out_shape=whole_out,
            in_specs=[SM, SM] + [VM] * (2 + len(pieces)) + [ANY] * len(extra),
            out_specs=ANY,
            scratch_shapes=SINK_SCRATCH,
            input_output_aliases={4 + len(pieces): 0} if extra else {},
            compiler_params=pltpu.CompilerParams(vmem_limit_bytes=SINK_LIMIT << 20),
            cost_estimate=cost(9 * 3 * 2 * 256 * 512**2 * len(steps), 24 << 20),
            name="sink_block",
        )(pos, sign, high, low, *pieces, *extra)
    return out[None]


def solution(mesh):
    finer = Mesh(mesh.devices.reshape(SIZES), AXES)
    return jax.shard_map(
        contract,
        mesh=finer,
        in_specs=(
            P(ROW, None, None, COL, None),
            P(None, None, AXES, None),
            P(None, COL, None, None, ROW),
            P(),
            P(),
        ),
        out_specs=P(ROW, COL, None, None, None),
        check_vma=False,
    )
```
